256 devices in a mesh: groups: 2 (over z), blk: 16 (over y, core), col: 8 (over x).
Axes of the slice: x: 8, y: 8, z: 2, core: 2. Of those that a mesh axis runs over, the one named last changes fastest.
The devices are a block of a 8x8x16 slice.
Arguments:
- pair_block: bfloat16 [4096, 16384], P(('groups', 'blk'), 'col'), parts along dimension 0, may hold values from -1.5 to 1.5
- occ_energy: float32 [2], P('groups'), parts along dimension 0, may hold values from -1.5 to -0.3
- virt_energy: float32 [4096], P('groups'), parts along dimension 0, may hold values from 0.2 to 3
- frequency: float32 [2], P('groups'), parts along dimension 0, may hold values from 0.2 to 2
Outputs:
- dielectric: float32 [32768, 16384], P(('groups', 'col'), 'blk'), parts along dimension 0
The draws below stay inside these ranges and needn't reach their ends.
There are 2 independent parts, one for each index of `groups`. The reference program is written for one: setup_inputs(seed, part) draws one part's arguments, and reference() takes and returns one part's arrays. A program takes and returns all parts, laid end to end along the dimension named above; each array names one. Nothing has to cross between parts.
All inputs are finite; a program needn't handle non-finite values.
Results may differ from the reference program's by a relative error of at most 0.0027.
Values may be sent and summed in bfloat16 or wider, within the bound.
A program may use at most 64 MiB of HBM per device.

```python
import math
import jax
import jax.numpy as jnp
from jax import lax

NAUX = 16384
NVIRT = 2048
NOCC = 1
NPAIR = 2048


def block_scale(rng, extent, split, low, largest):
    def one(dim, shards_of):
        steps = jax.random.uniform(jax.random.fold_in(jax.random.fold_in(rng, 6), dim), (shards_of,), jnp.float32, low / len(split), largest / len(split))
        return jnp.repeat(jnp.exp(steps), extent[dim] // shards_of).reshape((-1,) + (1,) * (len(extent) - dim - 1))

    level = one(*split[0])
    for cut in split[1:]:
        level = level * one(*cut)
    return level


def gaussian(own_key, shape, scale, limit, shards=(), held_as=jnp.bfloat16):
    values = scale * jax.random.normal(own_key, shape, jnp.float32)
    if shards:
        values = values * block_scale(own_key, shape, shards, -0.22, 0.18)
    return jnp.clip(values, -limit, limit).astype(held_as)


def setup_inputs(seed: int = 0, part: int = 0) -> dict:
    streams_of = jax.random.split(jax.random.key(seed), 5)
    part_splits = jax.random.split(jax.random.fold_in(streams_of[4], part), 5)
    pair_block = gaussian(part_splits[0], (NPAIR, NAUX), (0.7 * NPAIR ** -0.25), 1.5, ((0, 16), (1, 8)))
    occ_energy = jnp.clip(jax.random.uniform(part_splits[1], (NOCC,), jnp.float32, -1.5, -0.3), -1.5, -0.3)
    virt_energy = jnp.clip(jnp.exp(jax.random.uniform(part_splits[2], (NVIRT,), jnp.float32, math.log(0.2), math.log(3.0))), 0.2, 3.0)
    frequency = jnp.clip(jnp.exp(jax.random.uniform(part_splits[3], (1,), jnp.float32, math.log(0.2), math.log(2.0))), 0.2, 2.0)
    return {"pair_block": pair_block, "occ_energy": occ_energy, "virt_energy": virt_energy, "frequency": frequency}


def reference(pair_block, occ_energy, virt_energy, frequency):
    gap = (virt_energy[None, :] - occ_energy[:, None]).reshape(-1)
    weights = 2.0 * gap / (gap * gap + frequency[0] * frequency[0])
    scaled = (pair_block.astype(jnp.float32) * weights[:, None]).astype(jnp.bfloat16)
    return lax.dot_general(scaled, pair_block, (((0,), (0,)), ((), ())), preferred_element_type=jnp.float32)
```

```python
import functools

import jax
import jax.numpy as jnp
from jax import lax
from jax.experimental import pallas as pl
from jax.experimental.pallas import tpu as pltpu
from jax.sharding import PartitionSpec as P

MESH = pl.DeviceIdType.MESH
CORES = 2
SUB = 4
LAG = 4
HOP = 2


def element(e, up, row, n):
    half = SUB
    g = e + half
    dist, within = g // (CORES * SUB), g % (CORES * SUB)
    sub = within // CORES - jnp.where(dist == 0, SUB // 2, 0)
    sub = jnp.where(up, sub, SUB - 1 - sub)
    chip = (row + jnp.where(up, n - dist, dist)) % n
    return chip, sub, within % CORES


def schedule(n):
    total = n * CORES * SUB
    end = total // 2 + n // 2 * HOP
    table = []
    for pos in range(n):
        ready = {}
        for d in range(-(n // 2 - 1), n // 2 + 1):
            if d == 0:
                ready[d] = 1
            elif d == n // 2:
                ready[d] = LAG + 1 + 2 * (SUB * (n // 2 - 1) + SUB // 2 - 1)
            else:
                ready[d] = LAG + 1 + 2 * (SUB * abs(d) - 1)
        if pos:
            for e in range(total // 2):
                g = e + SUB
                dist = g // (CORES * SUB)
                for up in (True, False):
                    first, last = (pos, n - pos) if up else (n - pos, pos)
                    tick = e + first * HOP if e + first * HOP < end else total - 1 - e + last * HOP
                    key = dist if up else -dist
                    if dist == n // 2:
                        key = dist
                    ready[key] = max(ready[key], tick)
        order = sorted(ready, key=lambda d: (ready[d], abs(d), d))
        starts, free = [], 0
        for d in order[:-1]:
            free = max(free, ready[d])
            starts.append(free)
            free += 2
        table.append((order, starts))
    return end, table


def pick(index, values):
    out = jnp.int32(values[0])
    for k in range(1, len(values)):
        out = jnp.where(index == k, jnp.int32(values[k]), out)
    return out


def gather_kernel(n, block_ref, weight_ref, acc, last_lhs, last_rhs, held, load_sem,
                  y_send, y_recv, d_send, d_recv, x_send, x_recv):
    rows, cols = block_ref.shape
    piece = rows // SUB
    slab = cols // CORES
    tile = CORES * rows
    tiles = cols // tile
    b = lax.axis_index("blk")
    x = lax.axis_index("col")
    core, y = b % CORES, b // CORES
    other = 1 - core
    total = n * CORES * SUB
    end, table = schedule(n)
    send_end = end - HOP
    y_count = SUB * (n // 2 - 1) + SUB // 2
    pos = (x - y + n) % n

    peer = {"blk": y * CORES + other}
    chip_y = ({"blk": ((y + 1) % n) * CORES + core}, {"blk": ((y + n - 1) % n) * CORES + core})
    chip_x = ({"col": (x + 1) % n}, {"col": (x + n - 1) % n})

    load = pltpu.make_async_copy(
        block_ref, held.at[y, pl.ds(pl.multiple_of(core * rows, rows), rows), pl.ds(0, cols)], load_sem)
    load.start()
    barrier = pltpu.get_barrier_semaphore()
    for device in (peer,) + chip_y + chip_x:
        pl.semaphore_signal(barrier, inc=1, device_id=device, device_id_type=MESH)
    pl.semaphore_wait(barrier, 5)
    load.wait()

    def rows_of(owner, sub):
        return pl.ds(pl.multiple_of(owner * rows + sub * piece, piece), piece)

    def full(chip, owner, sub):
        return held.at[chip, rows_of(owner, sub), pl.ds(0, cols)]

    def copy(src, dst, send, recv, device):
        return pltpu.make_async_remote_copy(src_ref=src, dst_ref=dst, send_sem=send, recv_sem=recv,
                                            device_id=device, device_id_type=MESH)

    def y_copy(way, j):
        d, k = j // SUB, j % SUB
        chip = (y + (n - d if way == 0 else d)) % n
        ref = full(chip, core, k if way == 0 else SUB - 1 - k)
        return copy(ref, ref, y_send.at[way, j], y_recv.at[way, j], chip_y[way])

    def y_arrival(way, j):
        d, k = j // SUB + 1, j % SUB
        chip = (y + (n - d if way == 0 else d)) % n
        return chip, k if way == 0 else SUB - 1 - k

    def d_copy(way, j, owner):
        chip, sub = y_arrival(way, j)
        ref = full(chip, owner, sub)
        return copy(ref, ref, d_send.at[way, j], d_recv.at[way, j], peer)

    def own_copy(k, owner):
        ref = full(y, owner, k)
        return copy(ref, ref, d_send.at[2, k], d_recv.at[2, k], peer)

    for k in range(SUB):
        for way in (0, 1):
            y_copy(way, k).start()
    for k in range(SUB):
        own_copy(k, core).start()

    zero = jnp.zeros((tile, slab), jnp.float32)

    def clear(m, carry):
        acc[pl.ds(pl.multiple_of(m * tile, tile), tile), :] = zero
        return carry

    lax.fori_loop(0, tiles, clear, 0)

    landing = pl.ds(cols, slab)
    source = pl.ds(pl.multiple_of(jnp.where(pos == 0, core * slab, cols), slab), slab)
    hops = (pos, (n - pos) % n)

    def x_copy(way, i):
        up = (i < total // 2) if way == 0 else (i >= total // 2)
        chip, sub, swap = element(jnp.where(i < total // 2, i, total - 1 - i), up, y, n)
        owner = (core + swap) % CORES
        at = rows_of(owner, sub)
        return copy(held.at[chip, at, source], held.at[chip, at, landing],
                    x_send.at[way, i], x_recv.at[way, i], chip_x[way])

    def x_sends(way, t):
        i = t - hops[way] * HOP
        return (i >= 0) & (t < send_end) & (hops[way] != n - 1), i

    def x_step(t):
        for way in (0, 1):
            i = t - hops[way] * HOP

            @pl.when((i >= 0) & (t < end) & (hops[way] != 0))
            def _():
                x_copy(way, i).wait_recv()

            @pl.when((i >= 0) & (t < send_end) & (hops[way] != n - 1))
            def _():
                x_copy(way, i).start()

    order = [pick(pos, [o[s] for o, _ in table]) for s in range(n)]
    starts = [pick(pos, [s[k] for _, s in table]) for k in range(n - 1)]
    steps = max(s[-1] for _, s in table) + 2
    steps += steps % 2

    def scaled(chip, m):
        part = held[chip, :, pl.ds(pl.multiple_of(m * tile, tile), tile)].T
        return (part.astype(jnp.float32) * weight_ref[pl.ds(chip, 1), :]).astype(jnp.bfloat16)

    def multiply(t):
        work = jnp.int32(-1)
        dist = jnp.int32(0)
        for k in range(n - 1):
            here = (t == starts[k]) | (t == starts[k] + 1)
            work = jnp.where(here, t - starts[k], work)
            dist = jnp.where(here, order[k], dist)

        @pl.when(work >= 0)
        def _():
            chip = (y + n - dist) % n

            def one(m, carry):
                at = pl.ds(pl.multiple_of(m * tile, tile), tile)
                acc[at, :] += jnp.dot(scaled(chip, m), held[chip, :, source], preferred_element_type=jnp.float32)
                return carry

            lax.fori_loop(work * (tiles // 2), (work + 1) * (tiles // 2), one, 0)

    final = (y + n - order[n - 1]) % n

    def pair(h, carry):
        t = 2 * h
        j = h - LAG // 2

        @pl.when((j >= 0) & (j < y_count))
        def _():
            for way in (0, 1):
                y_copy_in = d_copy(way, j, core)
                chip, sub = y_arrival(way, j)
                ref = full(chip, core, sub)
                copy(ref, ref, y_send.at[way, j], y_recv.at[way, j], chip_y[way]).wait_recv()

                @pl.when(j + SUB < y_count)
                def _():
                    y_copy(way, j + SUB).start()

                y_copy_in.start()

        x_step(t)
        multiply(t)

        @pl.when(h == 0)
        def _():
            for k in range(SUB):
                own_copy(k, other).wait_recv()

        @pl.when((j >= 0) & (j < y_count))
        def _():
            for way in (0, 1):
                d_copy(way, j, other).wait_recv()

        x_step(t + 1)
        multiply(t + 1)

        @pl.when(h == (end - 4) // 2)
        def _():
            def one(m, carry):
                last_lhs[pl.ds(pl.multiple_of(m * tile, tile), tile), :] = scaled(final, m)
                return carry

            lax.fori_loop(0, tiles, one, 0)

        return carry

    lax.fori_loop(0, steps // 2, pair, 0)
    last_rhs[...] = held[final, :, source]

    def drain_y(j, carry):
        for way in (0, 1):
            y_copy(way, j).wait_send()
            d_copy(way, j, core).wait_send()
        return carry

    lax.fori_loop(0, y_count, drain_y, 0)
    for k in range(SUB):
        own_copy(k, core).wait_send()

    def drain_x(t, carry):
        for way in (0, 1):
            sent, i = x_sends(way, t)

            @pl.when(sent)
            def _():
                x_copy(way, i).wait_send()
        return carry

    lax.fori_loop(0, send_end, drain_x, 0)


def finish_kernel(acc, lhs, rhs, out_ref, staged, sems):
    tiles = sems.shape[0]
    tile = acc.shape[0] // tiles
    copies = []
    for m in range(tiles):
        at = pl.ds(m * tile, tile)
        staged[at, :] = acc[at, :] + jnp.dot(lhs[at, :], rhs[...], preferred_element_type=jnp.float32)
        out = pltpu.make_async_copy(staged.at[at], out_ref.at[at], sems.at[m])
        out.start()
        copies.append(out)
    for out in copies:
        out.wait()


def shards(pair_block, occ_energy, virt_energy, frequency):
    rows, cols = pair_block.shape
    n = lax.axis_size("col")
    assert lax.axis_size("blk") == CORES * n
    slab = cols // CORES
    tile = CORES * rows
    gap = (virt_energy[None, :] - occ_energy[:, None]).reshape(-1)
    weights = (2.0 * gap / (gap * gap + frequency[0] * frequency[0])).reshape(n, tile)
    end, _ = schedule(n)
    y_count = SUB * (n // 2 - 1) + SUB // 2
    dma = pltpu.SemaphoreType.DMA
    vmem = pl.BlockSpec(memory_space=pltpu.VMEM)
    acc, lhs, rhs = pl.pallas_call(
        functools.partial(gather_kernel, n),
        out_shape=(pltpu.VMEM((cols, slab), jnp.float32), pltpu.VMEM((cols, tile), jnp.bfloat16),
                   pltpu.VMEM((tile, slab), jnp.bfloat16)),
        in_specs=[pl.BlockSpec(memory_space=pl.ANY), vmem],
        out_specs=(vmem, vmem, vmem),
        scratch_shapes=[
            pltpu.VMEM((n, tile, cols + slab), jnp.bfloat16),
            dma,
            dma((2, y_count)), dma((2, y_count)),
            dma((3, y_count)), dma((3, y_count)),
            dma((2, end)), dma((2, end)),
        ],
        compiler_params=pltpu.CompilerParams(collective_id=0, has_side_effects=True, vmem_limit_bytes=20 * 2**20),
    )(pair_block, weights)
    return pl.pallas_call(
        finish_kernel,
        out_shape=jax.ShapeDtypeStruct((cols, slab), jnp.float32),
        in_specs=[vmem, vmem, vmem],
        out_specs=pl.BlockSpec(memory_space=pl.ANY),
        scratch_shapes=[pltpu.VMEM((cols, slab), jnp.float32), dma((n,))],
        compiler_params=pltpu.CompilerParams(vmem_limit_bytes=20 * 2**20),
    )(acc, lhs, rhs)


def solution(mesh):
    return jax.shard_map(
        shards,
        mesh=mesh,
        in_specs=(P(("groups", "blk"), "col"), P("groups"), P("groups"), P("groups")),
        out_specs=P(("groups", "col"), "blk"),
        check_vma=False,
    )
```

```python
import functools

import jax
import jax.numpy as jnp
from jax import lax
from jax.experimental import pallas as pl
from jax.experimental.pallas import tpu as pltpu
from jax.sharding import PartitionSpec as P

MESH = pl.DeviceIdType.MESH
CORES = 2
SUB = 8
HOP = 4
LAG = 4
PASS = 2
PARTS = 2
RING = 8


def counts(n):
    total = n * SUB * 2
    return total, total // 2 + n // 2 * HOP, SUB * (n // 2 - 1) + SUB // 2


def element(e, up, row, n):
    wide = 2 * SUB
    g = e + wide // 2
    dist = g // wide
    sub = g % wide - jnp.where(dist == 0, wide // 2, 0)
    return (row + jnp.where(up, n - dist, dist)) % n, jnp.where(up, sub, wide - 1 - sub)


def schedule(n, core):
    total, end, y_count = counts(n)
    wide = 2 * SUB
    table = []
    for pos in range(n):
        ready = {0: 2}
        for d in range(1, n // 2):
            ready[d] = ready[-d] = LAG + SUB * d
        ready[n // 2] = LAG + y_count
        if pos:
            for e in range(total // 2):
                dist = (e + wide // 2) // wide
                for way in (0, 1):
                    hops = (pos, n - pos) if way == 0 else (n - pos, pos)
                    direct = e + hops[0] * HOP < end
                    tick = e + hops[0] * HOP if direct else total - 1 - e + hops[1] * HOP
                    delay = 0 if (way == core) == direct else PASS
                    key = dist if way == 0 or dist == n // 2 else -dist
                    ready[key] = max(ready[key], tick // 2 + delay)
        order = sorted(ready, key=lambda d: (ready[d], abs(d), d))
        starts, free = [], 0
        for d in order[:-1]:
            free = max(free, ready[d])
            starts.append(free)
            free += PARTS
        table.append((order, starts))
    return table


def pick(index, values):
    out = jnp.int32(values[0])
    for k in range(1, len(values)):
        out = jnp.where(index == k, jnp.int32(values[k]), out)
    return out


def gather_kernel(n, block_ref, occ_ref, virt_hbm, freq_ref, acc, last_lhs, last_rhs, held, weight, virt_ref, load_sem,
                  y_send, y_recv, d_send, d_recv, x_send, x_recv, h_send, h_recv, own_send, own_recv):
    rows, cols = block_ref.shape
    slab = cols // CORES
    tile = CORES * rows
    piece = tile // SUB
    fine = piece // 2
    tiles = cols // tile
    b = lax.axis_index("blk")
    x = lax.axis_index("col")
    core, y = b % CORES, b // CORES
    other = 1 - core
    total, end, y_count = counts(n)
    send_end = end - HOP
    pos = (x - y + n) % n

    def onward(place, way):
        return (place + jnp.where(way == 0, 1, n - 1)) % n

    peer = {"blk": y * CORES + other}
    chip_y = {"blk": onward(y, core) * CORES + core}
    chip_x = {"col": onward(x, core)}

    def own_rows(c):
        return held.at[y, pl.ds(pl.multiple_of(c * rows, rows), rows), pl.ds(0, cols)]

    load = pltpu.make_async_copy(block_ref, own_rows(core), load_sem.at[0])
    load.start()
    load_virt = pltpu.make_async_copy(virt_hbm, virt_ref, load_sem.at[1])
    load_virt.start()
    barrier = pltpu.get_barrier_semaphore()
    for device in (peer, chip_y, {"blk": onward(y, other) * CORES + core}, chip_x, {"col": onward(x, other)}):
        pl.semaphore_signal(barrier, inc=1, device_id=device, device_id_type=MESH)

    load_virt.wait()
    for k in range(n):
        virtuals = virt_ref.shape[1]
        gap = virt_ref[:, pl.ds(k * tile % virtuals, tile)] - occ_ref[k * tile // virtuals]
        weight[pl.ds(k, 1), :] = 2.0 * gap / (gap * gap + freq_ref[0] * freq_ref[0])

    pl.semaphore_wait(barrier, 5)
    load.wait()

    def copy(src, dst, send, recv, device):
        return pltpu.make_async_remote_copy(src_ref=src, dst_ref=dst, send_sem=send, recv_sem=recv,
                                            device_id=device, device_id_type=MESH)

    def own_copy(c):
        return copy(own_rows(c), own_rows(c), own_send, own_recv, peer)

    def y_piece(way, j, shift):
        d, k = j // SUB + shift, j % SUB
        chip = (y + jnp.where(way == 0, n - d, d)) % n
        at = pl.ds(pl.multiple_of(jnp.where(way == 0, k, SUB - 1 - k) * piece, piece), piece)
        return held.at[chip, at, pl.ds(0, cols)]

    def y_copy(j):
        ref = y_piece(core, j, 0)
        return copy(ref, ref, y_send.at[j % RING], y_recv.at[j], chip_y)

    def y_arrival(j):
        ref = y_piece(core, j, 1)
        return copy(ref, ref, y_send.at[j % RING], y_recv.at[j], chip_y)

    def d_copy(way, j):
        ref = y_piece(way, j, 1)
        return copy(ref, ref, d_send.at[j % RING], d_recv.at[j], peer)

    base = jnp.where(pos == 0, 0, cols)
    hops = jnp.where(core == 0, pos, (n - pos) % n)
    back = jnp.where(core == 0, (n - pos) % n, pos)

    def x_place(way, i):
        return element(jnp.where(i < total // 2, i, total - 1 - i), (i < total // 2) == (way == 0), y, n)

    def x_copy(i):
        chip, sub = x_place(core, i)
        at = pl.ds(pl.multiple_of(sub * fine, fine), fine)
        return copy(held.at[chip, at, pl.ds(pl.multiple_of(base, cols), cols)], held.at[chip, at, pl.ds(cols, cols)],
                    x_send.at[i % RING], x_recv.at[i], chip_x)

    def h_copy(way, q):
        chip, sub = x_place(way, 2 * q)
        at = pl.ds(pl.multiple_of(sub // 2 * piece, piece), piece)
        ref = held.at[chip, at, pl.ds(pl.multiple_of(cols + (1 - way) * slab, slab), slab)]
        return copy(ref, ref, h_send.at[q % RING], h_recv.at[q], peer)

    tables = [schedule(n, c) for c in range(CORES)]
    merged = [tables[c][p] for p in range(n) for c in range(CORES)]
    which = pos * CORES + core
    order = [pick(which, [o[s] for o, _ in merged]) for s in range(n)]
    starts = [pick(which, [s[k] for _, s in merged]) for k in range(n - 1)]
    prepare = LAG + 1 + y_count
    steps = max(max(s[-1] for _, s in merged) + PARTS, prepare + tiles, end // 2 + PASS)
    rhs_cols = pl.ds(pl.multiple_of(base + core * slab, slab), slab)
    final = (y + n - order[n - 1]) % n
    part = cols // PARTS

    def scaled(chip, at):
        values = held[chip, :, at].T
        return (values.astype(jnp.float32) * weight[pl.ds(chip, 1), :]).astype(jnp.bfloat16)

    def multiply(u):
        work = jnp.int32(-1)
        dist = jnp.int32(0)
        for k in range(n - 1):
            here = (u >= starts[k]) & (u < starts[k] + PARTS)
            work = jnp.where(here, u - starts[k], work)
            dist = jnp.where(here, order[k], dist)

        @pl.when(work >= 0)
        def _():
            chip = (y + n - dist) % n
            at = pl.ds(pl.multiple_of(work * part, part), part)
            acc[at, :] += jnp.dot(scaled(chip, at), held[chip, :, rhs_cols], preferred_element_type=jnp.float32)

        @pl.when((u >= prepare) & (u < prepare + tiles))
        def _():
            at = pl.ds(pl.multiple_of((u - prepare) * tile, tile), tile)
            last_lhs[at, :] = scaled(final, at)

    def x_step(t):
        i = t - hops * HOP

        @pl.when((i >= 0) & (t < end) & (hops != 0))
        def _():
            x_copy(i).wait_recv()

        @pl.when((i >= 0) & (t < send_end) & (hops != n - 1))
        def _():
            @pl.when(i >= RING)
            def _():
                x_copy(i - RING).wait_send()
            x_copy(i).start()

    own_count = SUB // CORES
    for k in range(own_count):
        y_copy(k).start()

    @pl.when(hops == 0)
    def _():
        for i in range(HOP):
            x_copy(i).start()

    own_copy(core).start()
    zero = jnp.zeros((tile, slab), jnp.float32)
    for m in range(tiles // 2):
        acc[pl.ds(m * tile, tile), :] = zero
    own_copy(other).wait_recv()
    for k in range(own_count, SUB):
        y_copy(k).start()
    for m in range(tiles // 2, tiles):
        acc[pl.ds(m * tile, tile), :] = zero

    def step(u, carry):
        j = u - LAG

        @pl.when((j >= 0) & (j < y_count))
        def _():
            y_arrival(j).wait_recv()

            @pl.when(j + SUB < y_count)
            def _():
                y_copy(j).wait_send()
                y_copy(j + SUB).start()

            @pl.when(j >= RING)
            def _():
                d_copy(core, j - RING).wait_send()
            d_copy(core, j).start()

        @pl.when((j >= 1) & (j <= y_count))
        def _():
            d_copy(other, j - 1).wait_recv()

        x_step(2 * u)
        x_step(2 * u + 1)
        q = u - hops * (HOP // 2)

        @pl.when((q >= 0) & (u < end // 2) & (hops != 0))
        def _():
            @pl.when(q >= RING)
            def _():
                h_copy(core, q - RING).wait_send()
            h_copy(core, q).start()

        r = u - PASS - back * (HOP // 2)

        @pl.when((r >= 0) & (u - PASS < end // 2) & (back != 0))
        def _():
            h_copy(other, r).wait_recv()

        multiply(u)
        return carry

    lax.fori_loop(HOP // 2, steps, step, 0)
    last_rhs[...] = held[final, :, rhs_cols]
    for k in range(1, RING + 1):
        y_copy(y_count - k).wait_send()
        d_copy(core, y_count - k).wait_send()

        @pl.when(hops != n - 1)
        def _():
            x_copy(send_end - hops * HOP - k).wait_send()

        @pl.when(hops != 0)
        def _():
            h_copy(core, end // 2 - hops * (HOP // 2) - k).wait_send()
    own_copy(core).wait_send()


def finish_kernel(acc, lhs, rhs, out_ref, staged, sems):
    tiles = sems.shape[0]
    tile = acc.shape[0] // tiles
    copies = []
    for m in range(tiles):
        at = pl.ds(m * tile, tile)
        staged[at, :] = acc[at, :] + jnp.dot(lhs[at, :], rhs[...], preferred_element_type=jnp.float32)
        out = pltpu.make_async_copy(staged.at[at], out_ref.at[at], sems.at[m])
        out.start()
        copies.append(out)
    for out in copies:
        out.wait()


def shards(pair_block, occ_energy, virt_energy, frequency):
    rows, cols = pair_block.shape
    n = lax.axis_size("col")
    assert lax.axis_size("blk") == CORES * n
    slab = cols // CORES
    tile = CORES * rows
    assert virt_energy.shape[0] % tile == 0
    total, end, y_count = counts(n)
    dma = pltpu.SemaphoreType.DMA
    vmem = pl.BlockSpec(memory_space=pltpu.VMEM)
    hbm = pl.BlockSpec(memory_space=pltpu.HBM)
    smem = pl.BlockSpec(memory_space=pltpu.SMEM)
    acc, lhs, rhs = pl.pallas_call(
        functools.partial(gather_kernel, n),
        out_shape=(pltpu.VMEM((cols, slab), jnp.float32), pltpu.VMEM((cols, tile), jnp.bfloat16),
                   pltpu.VMEM((tile, slab), jnp.bfloat16)),
        in_specs=[hbm, smem, hbm, smem],
        out_specs=(vmem, vmem, vmem),
        scratch_shapes=[
            pltpu.VMEM((n, tile, 2 * cols), jnp.bfloat16), pltpu.VMEM((n, tile), jnp.float32),
            pltpu.VMEM((1, virt_energy.shape[0]), jnp.float32), dma((2,)),
            dma((RING,)), dma((y_count,)),
            dma((RING,)), dma((y_count,)),
            dma((RING,)), dma((end,)),
            dma((RING,)), dma((end // 2,)),
            dma, dma,
        ],
        compiler_params=pltpu.CompilerParams(collective_id=0, has_side_effects=True, vmem_limit_bytes=26 * 2**20),
    )(pltpu.with_memory_space_constraint(pair_block, pltpu.HBM), occ_energy,
      pltpu.with_memory_space_constraint(virt_energy.reshape(1, -1), pltpu.HBM), frequency)
    return pl.pallas_call(
        finish_kernel,
        out_shape=jax.ShapeDtypeStruct((cols, slab), jnp.float32),
        in_specs=[vmem, vmem, vmem],
        out_specs=pl.BlockSpec(memory_space=pl.ANY),
        scratch_shapes=[pltpu.VMEM((cols, slab), jnp.float32), dma((n,))],
        compiler_params=pltpu.CompilerParams(vmem_limit_bytes=20 * 2**20),
    )(acc, lhs, rhs)


def solution(mesh):
    return jax.shard_map(
        shards,
        mesh=mesh,
        in_specs=(P(("groups", "blk"), "col"), P("groups"), P("groups"), P("groups")),
        out_specs=P(("groups", "col"), "blk"),
        check_vma=False,
    )
```

```python
import functools

import jax
import jax.numpy as jnp
from jax import lax
from jax.experimental import pallas as pl
from jax.experimental.pallas import tpu as pltpu
from jax.sharding import PartitionSpec as P

MESH = pl.DeviceIdType.MESH
CORES = 2
SUB = 8
HOP = 4
LAG = 4
PASS = 2
PARTS = 4
SHIFT = 2
RING = 8
PACE = 4.6


def counts(n):
    total = n * SUB * 2
    return total, total // 2 + n // 2 * HOP, SUB * (n // 2 - 1) + SUB // 2


def received(n, way, hops):
    return counts(n)[1] + (SHIFT if way else -SHIFT) - hops * HOP


def offset(hops):
    return 2 * round(hops * PACE / 2)


def low(value, size):
    return value & (size - 1)


def high(value, size):
    return value >> (size.bit_length() - 1)


def element(e, up, row, n):
    wide = 2 * SUB
    g = e + wide // 2
    dist = high(g, wide)
    sub = low(g, wide) - jnp.where(dist == 0, wide // 2, 0)
    return low(row + jnp.where(up, n - dist, dist), n), jnp.where(up, sub, wide - 1 - sub)


def schedule(n, core):
    total, end, y_count = counts(n)
    wide = 2 * SUB
    table = []
    for pos in range(n):
        ready = {0: 2}
        for d in range(1, n // 2):
            ready[d] = ready[-d] = LAG + SUB * d
        ready[n // 2] = LAG + y_count
        if pos:
            for e in range(total // 2):
                dist = (e + wide // 2) // wide
                for way in (0, 1):
                    hops = (pos, n - pos) if way == 0 else (n - pos, pos)
                    direct = e < received(n, way, hops[0])
                    tick = e + offset(hops[0]) if direct else total - 1 - e + offset(hops[1])
                    delay = 0 if (way == core) == direct else PASS
                    key = dist if way == 0 or dist == n // 2 else -dist
                    ready[key] = max(ready[key], tick // 2 + delay + 1)
        order = sorted(ready, key=lambda d: (ready[d], abs(d), d))
        starts, free = [], 0
        for d in order[:-1]:
            free = max(free, ready[d])
            starts.append(free)
            free += PARTS // 2
        table.append((order, starts))
    return table


def pick(index, values):
    out = jnp.int32(values[0])
    for k in range(1, len(values)):
        out = jnp.where(index == k, jnp.int32(values[k]), out)
    return out


def gather_kernel(n, block_ref, occ_ref, virt_hbm, freq_ref, acc, last_lhs, last_rhs, held, weight, virt_ref, load_sem,
                  y_send, y_recv, d_send, d_recv, x_send, x_recv, h_send, h_recv, own_send, own_recv):
    rows, cols = block_ref.shape
    slab = cols // CORES
    tile = CORES * rows
    piece = tile // SUB
    fine = piece // 2
    tiles = cols // tile
    b = lax.axis_index("blk")
    x = lax.axis_index("col")
    core, y = low(b, CORES), high(b, CORES)
    other = 1 - core
    total, end, y_count = counts(n)
    pos = low(x - y + n, n)

    def onward(place, way):
        return low(place + jnp.where(way == 0, 1, n - 1), n)

    peer = {"blk": y * CORES + other}
    chip_y = {"blk": onward(y, core) * CORES + core}
    chip_x = {"col": onward(x, core)}

    def own_rows(c):
        return held.at[y, pl.ds(pl.multiple_of(c * rows, rows), rows), pl.ds(0, cols)]

    load = pltpu.make_async_copy(block_ref, own_rows(core), load_sem.at[0])
    load.start()
    load_virt = pltpu.make_async_copy(virt_hbm, virt_ref, load_sem.at[1])
    load_virt.start()
    barrier = pltpu.get_barrier_semaphore()
    for device in (peer, chip_y, {"blk": onward(y, other) * CORES + core}, chip_x, {"col": onward(x, other)}):
        pl.semaphore_signal(barrier, inc=1, device_id=device, device_id_type=MESH)

    load_virt.wait()
    for k in range(n):
        virtuals = virt_ref.shape[1]
        gap = virt_ref[:, pl.ds(k * tile % virtuals, tile)] - occ_ref[k * tile // virtuals]
        weight[pl.ds(k, 1), :] = 2.0 * gap / (gap * gap + freq_ref[0] * freq_ref[0])

    pl.semaphore_wait(barrier, 5)
    load.wait()

    def copy(src, dst, send, recv, device):
        return pltpu.make_async_remote_copy(src_ref=src, dst_ref=dst, send_sem=send, recv_sem=recv,
                                            device_id=device, device_id_type=MESH)

    def own_copy(c):
        return copy(own_rows(c), own_rows(c), own_send, own_recv, peer)

    def y_piece(way, j, shift):
        d, k = high(j, SUB) + shift, low(j, SUB)
        chip = low(y + jnp.where(way == 0, n - d, d), n)
        at = pl.ds(pl.multiple_of(jnp.where(way == 0, k, SUB - 1 - k) * piece, piece), piece)
        return held.at[chip, at, pl.ds(0, cols)]

    def y_copy(j):
        ref = y_piece(core, j, 0)
        return copy(ref, ref, y_send.at[low(j, RING)], y_recv.at[j], chip_y)

    def y_arrival(j):
        ref = y_piece(core, j, 1)
        return copy(ref, ref, y_send.at[low(j, RING)], y_recv.at[j], chip_y)

    def d_copy(way, j):
        ref = y_piece(way, j, 1)
        return copy(ref, ref, d_send.at[low(j, RING)], d_recv.at[j], peer)

    base = jnp.where(pos == 0, 0, cols)
    hops = jnp.where(core == 0, pos, low(n - pos, n))
    back = jnp.where(core == 0, low(n - pos, n), pos)
    wait_off = pick(hops, [offset(h) for h in range(n)])
    back_off = pick(back, [offset(h) for h in range(n)])
    arriving = jnp.where(hops == 0, 0, received(n, 1, hops) - jnp.where(core == 0, 2 * SHIFT, 0))
    leaving = jnp.where(hops == n - 1, 0, received(n, 1, hops + 1) - jnp.where(core == 0, 2 * SHIFT, 0))
    handed = jnp.where(back == 0, 0, received(n, 1, back) - jnp.where(core == 1, 2 * SHIFT, 0))

    def x_place(way, i):
        return element(jnp.where(i < total // 2, i, total - 1 - i), (i < total // 2) == (way == 0), y, n)

    def x_copy(i, place, second):
        chip, sub = place
        at = pl.ds(pl.multiple_of((sub ^ second) * fine, fine), fine)
        return copy(held.at[chip, at, pl.ds(pl.multiple_of(base, cols), cols)], held.at[chip, at, pl.ds(cols, cols)],
                    x_send.at[low(i, RING)], x_recv.at[i], chip_x)

    def h_copy(way, q, place):
        chip, sub = place
        at = pl.ds(pl.multiple_of(high(sub, 2) * piece, piece), piece)
        ref = held.at[chip, at, pl.ds(pl.multiple_of(cols + (1 - way) * slab, slab), slab)]
        return copy(ref, ref, h_send.at[low(q, RING)], h_recv.at[q], peer)

    tables = [schedule(n, c) for c in range(CORES)]
    merged = [tables[c][p] for p in range(n) for c in range(CORES)]
    which = pos * CORES + core
    order = [pick(which, [o[s] for o, _ in merged]) for s in range(n)]
    starts = [pick(which, [s[k] for _, s in merged]) for k in range(n - 1)]
    prepare = LAG + 1 + y_count
    steps = max(max(s[-1] for _, s in merged) + PARTS // 2, prepare + tiles,
                max(received(n, w, h) + offset(h) for w in (0, 1) for h in range(1, n)) // 2 + PASS)
    rhs_cols = pl.ds(pl.multiple_of(base + core * slab, slab), slab)
    final = low(y + n - order[n - 1], n)
    part = cols // PARTS

    def scaled(chip, at):
        values = held[chip, :, at].T
        return (values.astype(jnp.float32) * weight[pl.ds(chip, 1), :]).astype(jnp.bfloat16)

    def due(u):
        work = jnp.int32(-1)
        dist = jnp.int32(0)
        for k in range(n - 1):
            here = (u >= starts[k]) & (u < starts[k] + PARTS // 2)
            work = jnp.where(here, u - starts[k], work)
            dist = jnp.where(here, order[k], dist)
        return work, low(y + n - dist, n)

    def multiply(work, chip, second):
        @pl.when(work >= 0)
        def _():
            at = pl.ds(pl.multiple_of((2 * work + second) * part, part), part)
            acc[at, :] += jnp.dot(scaled(chip, at), held[chip, :, rhs_cols], preferred_element_type=jnp.float32)

    def prepare_last(u):
        @pl.when((u >= prepare) & (u < prepare + tiles))
        def _():
            at = pl.ds(pl.multiple_of((u - prepare) * tile, tile), tile)
            last_lhs[at, :] = scaled(final, at)

    own_count = SUB // CORES
    for k in range(own_count):
        y_copy(k).start()

    @pl.when(hops == 0)
    def _():
        for i in range(HOP):
            x_copy(i, x_place(core, jnp.int32(i - i % 2)), i % 2).start()

    own_copy(core).start()
    zero = jnp.zeros((tile, slab), jnp.float32)
    for m in range(tiles // 2):
        acc[pl.ds(m * tile, tile), :] = zero
    own_copy(other).wait_recv()
    for k in range(own_count, SUB):
        y_copy(k).start()
    for m in range(tiles // 2, tiles):
        acc[pl.ds(m * tile, tile), :] = zero

    def step(u, carry):
        j = u - LAG

        @pl.when((j >= 0) & (j < y_count))
        def _():
            y_arrival(j).wait_recv()

            @pl.when(j + SUB < y_count)
            def _():
                y_copy(j).wait_send()
                y_copy(j + SUB).start()

            @pl.when(j >= RING)
            def _():
                d_copy(core, j - RING).wait_send()
            d_copy(core, j).start()

        @pl.when((j >= 1) & (j <= y_count))
        def _():
            d_copy(other, j - 1).wait_recv()

        work, chip = due(u)
        i = 2 * u - wait_off
        place = x_place(core, i)
        for second in (0, 1):
            @pl.when((i >= 0) & (i < arriving))
            def _():
                x_copy(i + second, place, second).wait_recv()

            @pl.when((i >= 0) & (i < leaving))
            def _():
                @pl.when(i >= RING)
                def _():
                    x_copy(i + second - RING, place, second).wait_send()
                x_copy(i + second, place, second).start()

            if second == 0:
                multiply(work, chip, 0)

        q = u - high(wait_off, 2)

        @pl.when((q >= 0) & (i < arriving))
        def _():
            @pl.when(q >= RING)
            def _():
                h_copy(core, q - RING, place).wait_send()
            h_copy(core, q, place).start()

        r = u - PASS - high(back_off, 2)

        @pl.when((r >= 0) & (2 * r < handed))
        def _():
            h_copy(other, r, x_place(other, 2 * r)).wait_recv()

        multiply(work, chip, 1)
        prepare_last(u)
        return carry

    lax.fori_loop(HOP // 2, steps, step, 0)
    last_rhs[...] = held[final, :, rhs_cols]
    here = (y, jnp.int32(0))
    for k in range(1, RING + 1):
        y_copy(y_count - k).wait_send()
        d_copy(core, y_count - k).wait_send()

        @pl.when(leaving > 0)
        def _():
            x_copy(leaving - k, here, 0).wait_send()

        @pl.when(arriving > 0)
        def _():
            h_copy(core, high(arriving, 2) - k, here).wait_send()
    own_copy(core).wait_send()


def finish_kernel(acc, lhs, rhs, out_ref, staged, sems):
    tiles = sems.shape[0]
    tile = acc.shape[0] // tiles
    copies = []
    for m in range(tiles):
        at = pl.ds(m * tile, tile)
        staged[at, :] = acc[at, :] + jnp.dot(lhs[at, :], rhs[...], preferred_element_type=jnp.float32)
        out = pltpu.make_async_copy(staged.at[at], out_ref.at[at], sems.at[m])
        out.start()
        copies.append(out)
    for out in copies:
        out.wait()


def shards(pair_block, occ_energy, virt_energy, frequency):
    rows, cols = pair_block.shape
    n = lax.axis_size("col")
    assert lax.axis_size("blk") == CORES * n
    slab = cols // CORES
    tile = CORES * rows
    assert virt_energy.shape[0] % tile == 0
    total, end, y_count = counts(n)
    dma = pltpu.SemaphoreType.DMA
    vmem = pl.BlockSpec(memory_space=pltpu.VMEM)
    hbm = pl.BlockSpec(memory_space=pltpu.HBM)
    smem = pl.BlockSpec(memory_space=pltpu.SMEM)
    acc, lhs, rhs = pl.pallas_call(
        functools.partial(gather_kernel, n),
        out_shape=(pltpu.VMEM((cols, slab), jnp.float32), pltpu.VMEM((cols, tile), jnp.bfloat16),
                   pltpu.VMEM((tile, slab), jnp.bfloat16)),
        in_specs=[hbm, smem, hbm, smem],
        out_specs=(vmem, vmem, vmem),
        scratch_shapes=[
            pltpu.VMEM((n, tile, 2 * cols), jnp.bfloat16), pltpu.VMEM((n, tile), jnp.float32),
            pltpu.VMEM((1, virt_energy.shape[0]), jnp.float32), dma((2,)),
            dma((RING,)), dma((y_count,)),
            dma((RING,)), dma((y_count,)),
            dma((RING,)), dma((end + SHIFT,)),
            dma((RING,)), dma(((end + SHIFT) // 2,)),
            dma, dma,
        ],
        compiler_params=pltpu.CompilerParams(collective_id=0, has_side_effects=True, vmem_limit_bytes=26 * 2**20),
    )(pltpu.with_memory_space_constraint(pair_block, pltpu.HBM), occ_energy,
      pltpu.with_memory_space_constraint(virt_energy.reshape(1, -1), pltpu.HBM), frequency)
    return pl.pallas_call(
        finish_kernel,
        out_shape=jax.ShapeDtypeStruct((cols, slab), jnp.float32),
        in_specs=[vmem, vmem, vmem],
        out_specs=pl.BlockSpec(memory_space=pl.ANY),
        scratch_shapes=[pltpu.VMEM((cols, slab), jnp.float32), dma((n,))],
        compiler_params=pltpu.CompilerParams(vmem_limit_bytes=20 * 2**20),
    )(acc, lhs, rhs)


def solution(mesh):
    return jax.shard_map(
        shards,
        mesh=mesh,
        in_specs=(P(("groups", "blk"), "col"), P("groups"), P("groups"), P("groups")),
        out_specs=P(("groups", "col"), "blk"),
        check_vma=False,
    )
```

```python
import functools

import jax
import jax.numpy as jnp
from jax import lax
from jax.experimental import pallas as pl
from jax.experimental.pallas import tpu as pltpu
from jax.sharding import PartitionSpec as P

MESH = pl.DeviceIdType.MESH
CORES = 2
SUB = 8
FINE = 2
HOP = 4
LAG = 4
PASS = 2
PARTS = 4
SHIFT = 2
RING = 8
X_RING = 8
PACE = 2.0
PARTNER_PACE = 2.4
EASE = 4


def counts(n):
    total = n * SUB * FINE
    return total, total // 2 + n // 2 * HOP, SUB * (n // 2 - 1) + SUB // 2


def received(n, way, hops):
    return counts(n)[1] + (SHIFT if way else -SHIFT) - hops * HOP


def offset(hops, pace=PACE):
    return FINE * round(hops * pace)


def low(value, size):
    return value & (size - 1)


def high(value, size):
    return value >> (size.bit_length() - 1)


def element(e, up, row, n):
    wide = FINE * SUB
    g = e + wide // 2
    dist = high(g, wide)
    sub = low(g, wide) - jnp.where(dist == 0, wide // 2, 0)
    return low(row + jnp.where(up, n - dist, dist), n), jnp.where(up, sub, wide - 1 - sub)


def schedule(n, core):
    total, end, y_count = counts(n)
    wide = FINE * SUB
    table = []
    for pos in range(n):
        ready = {0: 2}
        for d in range(1, n // 2):
            ready[d] = ready[-d] = LAG + SUB * d - 1 + (EASE if pos else 1)
        ready[n // 2] = LAG + y_count - 1 + (EASE if pos else 1)
        if pos:
            for e in range(total // 2):
                dist = (e + wide // 2) // wide
                for way in (0, 1):
                    hops = (pos, n - pos) if way == 0 else (n - pos, pos)
                    direct = e < received(n, way, hops[0])
                    mine = (way == core) == direct
                    hop = hops[0] if direct else hops[1]
                    tick = (e if direct else total - 1 - e) + offset(hop, PACE if mine else PARTNER_PACE)
                    delay = 0 if mine else PASS
                    key = dist if way == 0 or dist == n // 2 else -dist
                    ready[key] = max(ready[key], tick // FINE + delay + 1)
        order = sorted(ready, key=lambda d: (ready[d], abs(d), d))
        starts, free = [], 0
        for d in order[:-1]:
            free = max(free, ready[d])
            starts.append(free)
            free += PARTS // 2
        table.append((order, starts))
    return table


def pick(index, values):
    out = jnp.int32(values[0])
    for k in range(1, len(values)):
        out = jnp.where(index == k, jnp.int32(values[k]), out)
    return out


def gather_kernel(n, block_ref, occ_ref, virt_hbm, freq_ref, acc, last_lhs, last_rhs, held, weight, virt_ref, load_sem,
                  y_send, y_recv, d_send, d_recv, x_send, x_recv, h_send, h_recv, own_send, own_recv):
    rows, cols = block_ref.shape
    slab = cols // CORES
    tile = CORES * rows
    piece = tile // SUB
    fine = piece // FINE
    tiles = cols // tile
    b = lax.axis_index("blk")
    x = lax.axis_index("col")
    core, y = low(b, CORES), high(b, CORES)
    other = 1 - core
    total, end, y_count = counts(n)
    pos = low(x - y + n, n)

    def onward(place, way):
        return low(place + jnp.where(way == 0, 1, n - 1), n)

    peer = {"blk": y * CORES + other}
    chip_y = {"blk": onward(y, core) * CORES + core}
    chip_x = {"col": onward(x, core)}

    def own_rows(c):
        return held.at[y, pl.ds(pl.multiple_of(c * rows, rows), rows), pl.ds(0, cols)]

    load = pltpu.make_async_copy(block_ref, own_rows(core), load_sem.at[0])
    load.start()
    load_virt = pltpu.make_async_copy(virt_hbm, virt_ref, load_sem.at[1])
    load_virt.start()
    barrier = pltpu.get_barrier_semaphore()
    for device in (peer, chip_y, {"blk": onward(y, other) * CORES + core}, chip_x, {"col": onward(x, other)}):
        pl.semaphore_signal(barrier, inc=1, device_id=device, device_id_type=MESH)

    load_virt.wait()
    for k in range(n):
        virtuals = virt_ref.shape[1]
        gap = virt_ref[:, pl.ds(k * tile % virtuals, tile)] - occ_ref[k * tile // virtuals]
        weight[pl.ds(k, 1), :] = 2.0 * gap / (gap * gap + freq_ref[0] * freq_ref[0])

    pl.semaphore_wait(barrier, 5)
    load.wait()

    def copy(src, dst, send, recv, device):
        return pltpu.make_async_remote_copy(src_ref=src, dst_ref=dst, send_sem=send, recv_sem=recv,
                                            device_id=device, device_id_type=MESH)

    def own_copy(c):
        return copy(own_rows(c), own_rows(c), own_send, own_recv, peer)

    def y_piece(way, j, shift):
        d, k = high(j, SUB) + shift, low(j, SUB)
        chip = low(y + jnp.where(way == 0, n - d, d), n)
        at = pl.ds(pl.multiple_of(jnp.where(way == 0, k, SUB - 1 - k) * piece, piece), piece)
        return held.at[chip, at, pl.ds(0, cols)]

    def y_copy(j):
        ref = y_piece(core, j, 0)
        return copy(ref, ref, y_send.at[low(j, RING)], y_recv.at[j], chip_y)

    def y_arrival(j):
        ref = y_piece(core, j, 1)
        return copy(ref, ref, y_send.at[low(j, RING)], y_recv.at[j], chip_y)

    def d_copy(way, j):
        ref = y_piece(way, j, 1)
        return copy(ref, ref, d_send.at[low(j, RING)], d_recv.at[j], peer)

    base = jnp.where(pos == 0, 0, cols)
    hops = jnp.where(core == 0, pos, low(n - pos, n))
    back = jnp.where(core == 0, low(n - pos, n), pos)
    wait_off = pick(hops, [offset(h) for h in range(n)])
    back_off = pick(back, [offset(h, PARTNER_PACE) for h in range(n)])
    arriving = jnp.where(hops == 0, 0, received(n, 1, hops) - jnp.where(core == 0, 2 * SHIFT, 0))
    leaving = jnp.where(hops == n - 1, 0, received(n, 1, hops + 1) - jnp.where(core == 0, 2 * SHIFT, 0))
    handed = jnp.where(back == 0, 0, received(n, 1, back) - jnp.where(core == 1, 2 * SHIFT, 0))

    def x_place(way, i):
        return element(jnp.where(i < total // 2, i, total - 1 - i), (i < total // 2) == (way == 0), y, n)

    def x_copy(i, place, second):
        chip, sub = place
        at = pl.ds(pl.multiple_of((sub ^ second) * fine, fine), fine)
        return copy(held.at[chip, at, pl.ds(pl.multiple_of(base, cols), cols)], held.at[chip, at, pl.ds(cols, cols)],
                    x_send.at[low(i, X_RING)], x_recv.at[i], chip_x)

    def h_copy(way, q, place):
        chip, sub = place
        at = pl.ds(pl.multiple_of(high(sub, FINE) * piece, piece), piece)
        ref = held.at[chip, at, pl.ds(pl.multiple_of(cols + (1 - way) * slab, slab), slab)]
        return copy(ref, ref, h_send.at[low(q, RING)], h_recv.at[q], peer)

    tables = [schedule(n, c) for c in range(CORES)]
    merged = [tables[c][p] for p in range(n) for c in range(CORES)]
    which = pos * CORES + core
    order = [pick(which, [o[s] for o, _ in merged]) for s in range(n)]
    starts = [pick(which, [s[k] for _, s in merged]) for k in range(n - 1)]
    prepare = LAG + EASE + y_count
    last = []
    for p in range(n):
        for c in range(CORES):
            mine, theirs = (p, (n - p) % n) if c == 0 else ((n - p) % n, p)
            step_ends = [tables[c][p][1][-1] + PARTS // 2, prepare + tiles // 2]
            if mine < n - 1:
                step_ends.append((received(n, c, mine + 1) + offset(mine)) // FINE)
            if mine:
                step_ends.append((received(n, c, mine) + offset(mine)) // FINE)
            if theirs:
                step_ends.append((received(n, 1 - c, theirs) + offset(theirs, PARTNER_PACE)) // FINE + PASS)
            last.append(max(step_ends))
    steps = pick(which, last)
    rhs_cols = pl.ds(pl.multiple_of(base + core * slab, slab), slab)
    final = low(y + n - order[n - 1], n)
    part = cols // PARTS

    def scaled(chip, at):
        values = held[chip, :, at].T
        return (values.astype(jnp.float32) * weight[pl.ds(chip, 1), :]).astype(jnp.bfloat16)

    def due(u):
        work = jnp.int32(-1)
        dist = jnp.int32(0)
        for k in range(n - 1):
            here = (u >= starts[k]) & (u < starts[k] + PARTS // 2)
            work = jnp.where(here, u - starts[k], work)
            dist = jnp.where(here, order[k], dist)
        return work, low(y + n - dist, n)

    def multiply(work, chip, second):
        @pl.when(work >= 0)
        def _():
            at = pl.ds(pl.multiple_of((2 * work + second) * part, part), part)
            acc[at, :] += jnp.dot(scaled(chip, at), held[chip, :, rhs_cols], preferred_element_type=jnp.float32)

    def prepare_last(u):
        @pl.when((u >= prepare) & (u < prepare + tiles // 2))
        def _():
            for k in (0, 1):
                at = pl.ds(pl.multiple_of((2 * (u - prepare) + k) * tile, tile), tile)
                last_lhs[at, :] = scaled(final, at)

    own_count = SUB // CORES
    ease = jnp.where(pos == 0, 1, EASE)
    for k in range(own_count):
        y_copy(k).start()

    @pl.when(hops == 0)
    def _():
        for i in range(HOP):
            x_copy(i, x_place(core, jnp.int32(i - i % FINE)), i % FINE).start()

    own_copy(core).start()
    zero = jnp.zeros((tile, slab), jnp.float32)
    for m in range(tiles // 2):
        acc[pl.ds(m * tile, tile), :] = zero
    own_copy(other).wait_recv()
    for k in range(own_count, SUB):
        y_copy(k).start()
    for m in range(tiles // 2, tiles):
        acc[pl.ds(m * tile, tile), :] = zero

    def step(u, carry):
        j = u - LAG

        @pl.when((j >= 0) & (j < y_count))
        def _():
            y_arrival(j).wait_recv()

            @pl.when(j + SUB < y_count)
            def _():
                y_copy(j).wait_send()
                y_copy(j + SUB).start()

            @pl.when(j >= RING)
            def _():
                d_copy(core, j - RING).wait_send()
            d_copy(core, j).start()

        given = j - ease

        @pl.when((given >= 0) & (given < y_count))
        def _():
            d_copy(other, given).wait_recv()

        work, chip = due(u)
        i = FINE * u - wait_off
        place = x_place(core, i)
        for second in range(FINE):
            @pl.when((i >= 0) & (i < arriving))
            def _():
                x_copy(i + second, place, second).wait_recv()

            @pl.when((i >= 0) & (i < leaving))
            def _():
                @pl.when(i >= X_RING)
                def _():
                    x_copy(i + second - X_RING, place, second).wait_send()
                x_copy(i + second, place, second).start()

            if second == FINE // 2 - 1:
                multiply(work, chip, 0)

        q = u - high(wait_off, FINE)

        @pl.when((q >= 0) & (i < arriving))
        def _():
            @pl.when(q >= RING)
            def _():
                h_copy(core, q - RING, place).wait_send()
            h_copy(core, q, place).start()

        r = u - PASS - high(back_off, FINE)

        @pl.when((r >= 0) & (FINE * r < handed))
        def _():
            h_copy(other, r, x_place(other, FINE * r)).wait_recv()

        multiply(work, chip, 1)
        prepare_last(u)
        return carry

    lax.fori_loop(HOP // FINE, steps, step, 0)
    last_rhs[...] = held[final, :, rhs_cols]
    here = (y, jnp.int32(0))
    for k in range(1, RING + 1):
        y_copy(y_count - k).wait_send()
        d_copy(core, y_count - k).wait_send()

        @pl.when(arriving > 0)
        def _():
            h_copy(core, high(arriving, FINE) - k, here).wait_send()
    for k in range(1, X_RING + 1):
        @pl.when(leaving > 0)
        def _():
            x_copy(leaving - k, here, 0).wait_send()
    own_copy(core).wait_send()


def finish_kernel(acc, lhs, rhs, out_ref, staged, sems):
    tiles = sems.shape[0]
    tile = acc.shape[0] // tiles
    copies = []
    for m in range(tiles):
        at = pl.ds(m * tile, tile)
        staged[at, :] = acc[at, :] + jnp.dot(lhs[at, :], rhs[...], preferred_element_type=jnp.float32)
        out = pltpu.make_async_copy(staged.at[at], out_ref.at[at], sems.at[m])
        out.start()
        copies.append(out)
    for out in copies:
        out.wait()


def shards(pair_block, occ_energy, virt_energy, frequency):
    rows, cols = pair_block.shape
    n = lax.axis_size("col")
    assert lax.axis_size("blk") == CORES * n
    slab = cols // CORES
    tile = CORES * rows
    assert virt_energy.shape[0] % tile == 0
    total, end, y_count = counts(n)
    dma = pltpu.SemaphoreType.DMA
    vmem = pl.BlockSpec(memory_space=pltpu.VMEM)
    hbm = pl.BlockSpec(memory_space=pltpu.HBM)
    smem = pl.BlockSpec(memory_space=pltpu.SMEM)
    acc, lhs, rhs = pl.pallas_call(
        functools.partial(gather_kernel, n),
        out_shape=(pltpu.VMEM((cols, slab), jnp.float32), pltpu.VMEM((cols, tile), jnp.bfloat16),
                   pltpu.VMEM((tile, slab), jnp.bfloat16)),
        in_specs=[hbm, smem, hbm, smem],
        out_specs=(vmem, vmem, vmem),
        scratch_shapes=[
            pltpu.VMEM((n, tile, 2 * cols), jnp.bfloat16), pltpu.VMEM((n, tile), jnp.float32),
            pltpu.VMEM((1, virt_energy.shape[0]), jnp.float32), dma((2,)),
            dma((RING,)), dma((y_count,)),
            dma((RING,)), dma((y_count,)),
            dma((X_RING,)), dma((end + SHIFT,)),
            dma((RING,)), dma(((end + SHIFT) // FINE,)),
            dma, dma,
        ],
        compiler_params=pltpu.CompilerParams(collective_id=0, has_side_effects=True, vmem_limit_bytes=26 * 2**20),
    )(pltpu.with_memory_space_constraint(pair_block, pltpu.HBM), occ_energy,
      pltpu.with_memory_space_constraint(virt_energy.reshape(1, -1), pltpu.HBM), frequency)
    return pl.pallas_call(
        finish_kernel,
        out_shape=jax.ShapeDtypeStruct((cols, slab), jnp.float32),
        in_specs=[vmem, vmem, vmem],
        out_specs=pl.BlockSpec(memory_space=pl.ANY),
        scratch_shapes=[pltpu.VMEM((cols, slab), jnp.float32), dma((n,))],
        compiler_params=pltpu.CompilerParams(vmem_limit_bytes=20 * 2**20),
    )(acc, lhs, rhs)


def solution(mesh):
    return jax.shard_map(
        shards,
        mesh=mesh,
        in_specs=(P(("groups", "blk"), "col"), P("groups"), P("groups"), P("groups")),
        out_specs=P(("groups", "col"), "blk"),
        check_vma=False,
    )
```

```python
import functools

import jax
import jax.numpy as jnp
from jax import lax
from jax.experimental import pallas as pl
from jax.experimental.pallas import tpu as pltpu
from jax.sharding import PartitionSpec as P

MESH = pl.DeviceIdType.MESH
CORES = 2
SUB = 8
FINE = 2
HOP = 4
LAG = 4
PASS = 1
PARTS = 4
SHIFT = 4
RING = 8
X_RING = 8
PACE = 2.0
PARTNER_PACE = 2.5
EASE = 4


def counts(n):
    total = n * SUB * FINE
    return total, total // 2 + n // 2 * HOP, SUB * (n // 2 - 1) + SUB // 2


def received(n, way, hops):
    return counts(n)[1] + (SHIFT if way else -SHIFT) - hops * HOP


def offset(hops, pace=PACE):
    return FINE * round(hops * pace)


def low(value, size):
    return value & (size - 1)


def high(value, size):
    return value >> (size.bit_length() - 1)


def element(e, up, row, n):
    wide = FINE * SUB
    g = e + wide // 2
    dist = high(g, wide)
    sub = low(g, wide) - jnp.where(dist == 0, wide // 2, 0)
    return low(row + jnp.where(up, n - dist, dist), n), jnp.where(up, sub, wide - 1 - sub)


def schedule(n, core):
    total, end, y_count = counts(n)
    wide = FINE * SUB
    table = []
    for pos in range(n):
        ready = {0: 2}
        for d in range(1, n // 2):
            ready[d] = ready[-d] = LAG + SUB * d - 1 + (EASE if pos else 1)
        ready[n // 2] = LAG + y_count - 1 + (EASE if pos else 1)
        if pos:
            for e in range(total // 2):
                dist = (e + wide // 2) // wide
                for way in (0, 1):
                    hops = (pos, n - pos) if way == 0 else (n - pos, pos)
                    direct = e < received(n, way, hops[0])
                    mine = (way == core) == direct
                    hop = hops[0] if direct else hops[1]
                    tick = (e if direct else total - 1 - e) + offset(hop, PACE if mine else PARTNER_PACE)
                    delay = 0 if mine else PASS
                    key = dist if way == 0 or dist == n // 2 else -dist
                    ready[key] = max(ready[key], tick // FINE + delay + 1)
        order = sorted(ready, key=lambda d: (ready[d], abs(d), d))
        starts, free = [], 0
        for d in order[:-1]:
            free = max(free, ready[d])
            starts.append(free)
            free += PARTS // 2
        table.append((order, starts))
    return table


def pick(index, values):
    out = jnp.int32(values[0])
    for k in range(1, len(values)):
        out = jnp.where(index == k, jnp.int32(values[k]), out)
    return out


def gather_kernel(n, block_ref, occ_ref, virt_hbm, freq_ref, acc, last_lhs, last_rhs, held, weight, virt_ref, load_sem,
                  y_send, y_recv, d_send, d_recv, x_send, x_recv, h_send, h_recv, own_send, own_recv):
    rows, cols = block_ref.shape
    slab = cols // CORES
    tile = CORES * rows
    piece = tile // SUB
    fine = piece // FINE
    tiles = cols // tile
    b = lax.axis_index("blk")
    x = lax.axis_index("col")
    core, y = low(b, CORES), high(b, CORES)
    other = 1 - core
    total, end, y_count = counts(n)
    pos = low(x - y + n, n)

    def onward(place, way):
        return low(place + jnp.where(way == 0, 1, n - 1), n)

    peer = {"blk": y * CORES + other}
    chip_y = {"blk": onward(y, core) * CORES + core}
    chip_x = {"col": onward(x, core)}

    def own_rows(c):
        return held.at[y, pl.ds(pl.multiple_of(c * rows, rows), rows), pl.ds(0, cols)]

    load = pltpu.make_async_copy(block_ref, own_rows(core), load_sem.at[0])
    load.start()
    load_virt = pltpu.make_async_copy(virt_hbm, virt_ref, load_sem.at[1])
    load_virt.start()
    barrier = pltpu.get_barrier_semaphore()
    for device in (peer, chip_y, {"blk": onward(y, other) * CORES + core}, chip_x, {"col": onward(x, other)}):
        pl.semaphore_signal(barrier, inc=1, device_id=device, device_id_type=MESH)

    load_virt.wait()
    for k in range(n):
        virtuals = virt_ref.shape[1]
        gap = virt_ref[:, pl.ds(k * tile % virtuals, tile)] - occ_ref[k * tile // virtuals]
        weight[pl.ds(k, 1), :] = 2.0 * gap / (gap * gap + freq_ref[0] * freq_ref[0])

    pl.semaphore_wait(barrier, 5)
    load.wait()

    def copy(src, dst, send, recv, device):
        return pltpu.make_async_remote_copy(src_ref=src, dst_ref=dst, send_sem=send, recv_sem=recv,
                                            device_id=device, device_id_type=MESH)

    def own_copy(c):
        return copy(own_rows(c), own_rows(c), own_send, own_recv, peer)

    def y_piece(way, j, shift):
        d, k = high(j, SUB) + shift, low(j, SUB)
        chip = low(y + jnp.where(way == 0, n - d, d), n)
        at = pl.ds(pl.multiple_of(jnp.where(way == 0, k, SUB - 1 - k) * piece, piece), piece)
        return held.at[chip, at, pl.ds(0, cols)]

    def y_copy(j):
        ref = y_piece(core, j, 0)
        return copy(ref, ref, y_send.at[low(j, RING)], y_recv.at[j], chip_y)

    def y_arrival(j):
        ref = y_piece(core, j, 1)
        return copy(ref, ref, y_send.at[low(j, RING)], y_recv.at[j], chip_y)

    def d_copy(way, j):
        ref = y_piece(way, j, 1)
        return copy(ref, ref, d_send.at[low(j, RING)], d_recv.at[j], peer)

    base = jnp.where(pos == 0, 0, cols)
    hops = jnp.where(core == 0, pos, low(n - pos, n))
    back = jnp.where(core == 0, low(n - pos, n), pos)
    wait_off = pick(hops, [offset(h) for h in range(n)])
    back_off = pick(back, [offset(h, PARTNER_PACE) for h in range(n)])
    arriving = jnp.where(hops == 0, 0, received(n, 1, hops) - jnp.where(core == 0, 2 * SHIFT, 0))
    leaving = jnp.where(hops == n - 1, 0, received(n, 1, hops + 1) - jnp.where(core == 0, 2 * SHIFT, 0))
    handed = jnp.where(back == 0, 0, received(n, 1, back) - jnp.where(core == 1, 2 * SHIFT, 0))

    def x_place(way, i):
        return element(jnp.where(i < total // 2, i, total - 1 - i), (i < total // 2) == (way == 0), y, n)

    def x_copy(i, place, second):
        chip, sub = place
        at = pl.ds(pl.multiple_of((sub ^ second) * fine, fine), fine)
        return copy(held.at[chip, at, pl.ds(pl.multiple_of(base, cols), cols)], held.at[chip, at, pl.ds(cols, cols)],
                    x_send.at[low(i, X_RING)], x_recv.at[i], chip_x)

    def h_copy(way, q, place):
        chip, sub = place
        at = pl.ds(pl.multiple_of(high(sub, FINE) * piece, piece), piece)
        ref = held.at[chip, at, pl.ds(pl.multiple_of(cols + (1 - way) * slab, slab), slab)]
        return copy(ref, ref, h_send.at[low(q, RING)], h_recv.at[q], peer)

    tables = [schedule(n, c) for c in range(CORES)]
    merged = [tables[c][p] for p in range(n) for c in range(CORES)]
    which = pos * CORES + core
    order = [pick(which, [o[s] for o, _ in merged]) for s in range(n)]
    starts = [pick(which, [s[k] for _, s in merged]) for k in range(n - 1)]
    prepare = LAG + EASE + y_count
    last = []
    for p in range(n):
        for c in range(CORES):
            mine, theirs = (p, (n - p) % n) if c == 0 else ((n - p) % n, p)
            step_ends = [tables[c][p][1][-1] + PARTS // 2, prepare + tiles // 2]
            if mine < n - 1:
                step_ends.append((received(n, c, mine + 1) + offset(mine)) // FINE)
            if mine:
                step_ends.append((received(n, c, mine) + offset(mine)) // FINE)
            if theirs:
                step_ends.append((received(n, 1 - c, theirs) + offset(theirs, PARTNER_PACE)) // FINE + PASS)
            last.append(max(step_ends))
    steps = pick(which, last)
    rhs_cols = pl.ds(pl.multiple_of(base + core * slab, slab), slab)
    final = low(y + n - order[n - 1], n)
    part = cols // PARTS

    def scaled(chip, at):
        values = held[chip, :, at].T
        return (values.astype(jnp.float32) * weight[pl.ds(chip, 1), :]).astype(jnp.bfloat16)

    def due(u):
        work = jnp.int32(-1)
        dist = jnp.int32(0)
        for k in range(n - 1):
            here = (u >= starts[k]) & (u < starts[k] + PARTS // 2)
            work = jnp.where(here, u - starts[k], work)
            dist = jnp.where(here, order[k], dist)
        return work, low(y + n - dist, n)

    def multiply(work, chip, second):
        @pl.when(work >= 0)
        def _():
            at = pl.ds(pl.multiple_of((2 * work + second) * part, part), part)
            acc[at, :] += jnp.dot(scaled(chip, at), held[chip, :, rhs_cols], preferred_element_type=jnp.float32)

    def prepare_last(u):
        @pl.when((u >= prepare) & (u < prepare + tiles // 2))
        def _():
            for k in (0, 1):
                at = pl.ds(pl.multiple_of((2 * (u - prepare) + k) * tile, tile), tile)
                last_lhs[at, :] = scaled(final, at)

    own_count = SUB // CORES
    ease = jnp.where(pos == 0, 1, EASE)
    for k in range(own_count):
        y_copy(k).start()

    @pl.when(hops == 0)
    def _():
        for i in range(HOP):
            x_copy(i, x_place(core, jnp.int32(i - i % FINE)), i % FINE).start()

    own_copy(core).start()
    zero = jnp.zeros((tile, slab), jnp.float32)
    for m in range(tiles // 2):
        acc[pl.ds(m * tile, tile), :] = zero
    own_copy(other).wait_recv()
    for k in range(own_count, SUB):
        y_copy(k).start()
    for m in range(tiles // 2, tiles):
        acc[pl.ds(m * tile, tile), :] = zero

    def step(u, carry):
        j = u - LAG

        @pl.when((j >= 0) & (j < y_count))
        def _():
            y_arrival(j).wait_recv()

            @pl.when(j + SUB < y_count)
            def _():
                y_copy(j).wait_send()
                y_copy(j + SUB).start()

            @pl.when(j >= RING)
            def _():
                d_copy(core, j - RING).wait_send()
            d_copy(core, j).start()

        given = j - ease

        @pl.when((given >= 0) & (given < y_count))
        def _():
            d_copy(other, given).wait_recv()

        work, chip = due(u)
        i = FINE * u - wait_off
        place = x_place(core, i)
        for second in range(FINE):
            @pl.when((i >= 0) & (i < arriving))
            def _():
                x_copy(i + second, place, second).wait_recv()

            @pl.when((i >= 0) & (i < leaving))
            def _():
                @pl.when(i >= X_RING)
                def _():
                    x_copy(i + second - X_RING, place, second).wait_send()
                x_copy(i + second, place, second).start()

            if second == FINE // 2 - 1:
                multiply(work, chip, 0)

        q = u - high(wait_off, FINE)

        @pl.when((q >= 0) & (i < arriving))
        def _():
            @pl.when(q >= RING)
            def _():
                h_copy(core, q - RING, place).wait_send()
            h_copy(core, q, place).start()

        r = u - PASS - high(back_off, FINE)

        @pl.when((r >= 0) & (FINE * r < handed))
        def _():
            h_copy(other, r, x_place(other, FINE * r)).wait_recv()

        multiply(work, chip, 1)
        prepare_last(u)
        return carry

    lax.fori_loop(HOP // FINE, steps, step, 0)
    last_rhs[...] = held[final, :, rhs_cols]
    here = (y, jnp.int32(0))
    for k in range(1, RING + 1):
        y_copy(y_count - k).wait_send()
        d_copy(core, y_count - k).wait_send()

        @pl.when(arriving > 0)
        def _():
            h_copy(core, high(arriving, FINE) - k, here).wait_send()
    for k in range(1, X_RING + 1):
        @pl.when(leaving > 0)
        def _():
            x_copy(leaving - k, here, 0).wait_send()
    own_copy(core).wait_send()


def finish_kernel(acc, lhs, rhs, out_ref, staged, sems):
    tiles = sems.shape[0]
    tile = acc.shape[0] // tiles
    copies = []
    for m in range(tiles):
        at = pl.ds(m * tile, tile)
        staged[at, :] = acc[at, :] + jnp.dot(lhs[at, :], rhs[...], preferred_element_type=jnp.float32)
        out = pltpu.make_async_copy(staged.at[at], out_ref.at[at], sems.at[m])
        out.start()
        copies.append(out)
    for out in copies:
        out.wait()


def shards(pair_block, occ_energy, virt_energy, frequency):
    rows, cols = pair_block.shape
    n = lax.axis_size("col")
    assert lax.axis_size("blk") == CORES * n
    slab = cols // CORES
    tile = CORES * rows
    assert virt_energy.shape[0] % tile == 0
    total, end, y_count = counts(n)
    dma = pltpu.SemaphoreType.DMA
    vmem = pl.BlockSpec(memory_space=pltpu.VMEM)
    hbm = pl.BlockSpec(memory_space=pltpu.HBM)
    smem = pl.BlockSpec(memory_space=pltpu.SMEM)
    acc, lhs, rhs = pl.pallas_call(
        functools.partial(gather_kernel, n),
        out_shape=(pltpu.VMEM((cols, slab), jnp.float32), pltpu.VMEM((cols, tile), jnp.bfloat16),
                   pltpu.VMEM((tile, slab), jnp.bfloat16)),
        in_specs=[hbm, smem, hbm, smem],
        out_specs=(vmem, vmem, vmem),
        scratch_shapes=[
            pltpu.VMEM((n, tile, 2 * cols), jnp.bfloat16), pltpu.VMEM((n, tile), jnp.float32),
            pltpu.VMEM((1, virt_energy.shape[0]), jnp.float32), dma((2,)),
            dma((RING,)), dma((y_count,)),
            dma((RING,)), dma((y_count,)),
            dma((X_RING,)), dma((end + SHIFT,)),
            dma((RING,)), dma(((end + SHIFT) // FINE,)),
            dma, dma,
        ],
        compiler_params=pltpu.CompilerParams(collective_id=0, has_side_effects=True, vmem_limit_bytes=26 * 2**20),
    )(pltpu.with_memory_space_constraint(pair_block, pltpu.HBM), occ_energy,
      pltpu.with_memory_space_constraint(virt_energy.reshape(1, -1), pltpu.HBM), frequency)
    return pl.pallas_call(
        finish_kernel,
        out_shape=jax.ShapeDtypeStruct((cols, slab), jnp.float32),
        in_specs=[vmem, vmem, vmem],
        out_specs=pl.BlockSpec(memory_space=pl.ANY),
        scratch_shapes=[pltpu.VMEM((cols, slab), jnp.float32), dma((n,))],
        compiler_params=pltpu.CompilerParams(vmem_limit_bytes=20 * 2**20),
    )(acc, lhs, rhs)


def solution(mesh):
    return jax.shard_map(
        shards,
        mesh=mesh,
        in_specs=(P(("groups", "blk"), "col"), P("groups"), P("groups"), P("groups")),
        out_specs=P(("groups", "col"), "blk"),
        check_vma=False,
    )
```
